32 devices in a mesh: row: 8 (over z, y), basis: 4 (over x, core).
Axes of the slice: x: 2, y: 2, z: 4, core: 2. Of those that a mesh axis runs over, the one named last changes fastest.
Arguments:
- design: float32 [7680, 40960], P('row', 'basis'), may hold values from -0.029646354 to 0.029646354
- targets: float32 [7680], P('row'), may hold values from -6 to 6
- counts: int32 [7680, 128], P('row'), may hold values from 0 to 3
- coefficients: float32 [40960, 128], P('basis'), may hold values from -6 to 6
- step_size: float32 [128], replicated, may hold values from 0.03 to 0.15
Outputs:
- fitted: float32 [40960, 128], P('basis')
- influence: float32 [7680, 128], P('row')
The draws below stay inside these ranges and needn't reach their ends.
All inputs are finite; a program needn't handle non-finite values.
Results may differ from the reference program's by a relative error of at most 0.00017.
Values sent between devices are 32-bit elements; how exact they have to be, the bound alone decides.
No kernel may reach another device: no remote copies, remote signals or barrier semaphores. Data moves between devices by JAX's collectives and lax.ppermute only.
A program may use at most 128 MiB of HBM per device.

```python
import math
import jax
import jax.numpy as jnp
from jax import lax

BASIS = 40960
MEMBERS = 128
STEPS = 3
ROWS = 7680


def touch_ends(array, key, low, largest):
    dims = array.shape
    place = [jax.random.randint(jax.random.fold_in(key, axis), (), 0, dims[axis]) for axis in range(len(dims))]
    array = array.at[tuple(place)].set(low)
    longest = dims.index(max(dims))
    place[longest] = (place[longest] + 1) % dims[longest]
    return array.at[tuple(place)].set(largest)


def strengthened(array, rng, source, target, parts, factor):
    def block_of(dim):
        return (jnp.arange(array.shape[dim]) // (array.shape[dim] // parts)).reshape((-1,) + (1,) * (array.ndim - 1 - dim))

    first = jax.random.permutation(rng, parts)[block_of(target)]
    other_side = (block_of(target) + parts // 2) % parts
    return jnp.where((block_of(source) == first) | (block_of(source) == other_side), factor * array, array)


def steps_of(stream_key, shape, shards, low, top_value):
    def one(axis_at, parts):
        draws = jax.random.uniform(jax.random.fold_in(jax.random.fold_in(stream_key, 6), axis_at), (parts,), jnp.float32, low / len(shards), top_value / len(shards))
        return jnp.repeat(jnp.exp(draws), shape[axis_at] // parts).reshape((-1,) + (1,) * (len(shape) - axis_at - 1))

    gain = one(*shards[0])
    for cut in shards[1:]:
        gain = gain * one(*cut)
    return gain


def bell_draw(stream_key, dims, deviation, reach, shards=(), held_as=jnp.bfloat16):
    result = deviation * jax.random.normal(stream_key, dims, jnp.float32)
    if shards:
        result = result * steps_of(stream_key, dims, shards, -0.22, 0.18)
    return jnp.clip(result, -reach, reach).astype(held_as)


def noise_with(rng, extent, scale, most, split, heavy, dtype=jnp.bfloat16):
    entries = scale * jax.random.normal(rng, extent, jnp.float32)
    if split:
        entries = entries * steps_of(rng, extent, split, -0.22, 0.18)
    return jnp.clip(strengthened(entries, jax.random.fold_in(rng, 3), *heavy), -most, most).astype(dtype)


def setup_inputs(seed: int = 0) -> dict:
    splits = jax.random.split(jax.random.key(seed), 6)
    design = noise_with(splits[0], (ROWS, BASIS), (BASIS ** -0.5), 0.029646354, ((0, 8), (1, 4)), (0, 1, 8, 2.0), jnp.float32)
    targets = bell_draw(splits[1], (ROWS,), 1.0, 6.0, ((0, 8),), jnp.float32)
    counts = touch_ends(jax.random.randint(splits[2], (ROWS, MEMBERS), 0, 4), jax.random.fold_in(splits[2], 1), 0, 3).astype(jnp.int32)
    coefficients = bell_draw(splits[3], (BASIS, MEMBERS), 1.0, 6.0, ((0, 4),), jnp.float32)
    step_size = jnp.clip(jnp.exp(jax.random.uniform(splits[4], (MEMBERS,), jnp.float32, math.log(0.03), math.log(0.15))), 0.03, 0.15)
    return dict(design=design, targets=targets, counts=counts, coefficients=coefficients, step_size=step_size)


HIGH = lax.Precision.HIGHEST

def transposed(left, right):
    return lax.dot_general(left, right, (((0,), (0,)), ((), ())), precision=HIGH, preferred_element_type=jnp.float32)

def reference(design, targets, counts, coefficients, step_size):
    weights = counts.astype(jnp.float32)
    curvature = transposed(design * design, weights) + 0.01
    fitted = coefficients
    influence = jnp.zeros((design.shape[0], coefficients.shape[1]), jnp.float32)
    for step in range(STEPS):
        predicted = jnp.dot(design, fitted, precision=HIGH, preferred_element_type=jnp.float32)
        residual = predicted - targets[:, None]
        influence = weights * residual / jnp.sqrt(1.0 + residual * residual)
        gradient = transposed(design, influence)
        fitted = fitted - step_size[None, :] * gradient / curvature
    return (fitted, influence)
```

```python
import functools

import jax
import jax.numpy as jnp
from jax import lax
from jax.experimental import pallas as pl
from jax.experimental.pallas import tpu as pltpu
from jax.sharding import PartitionSpec as P


STEPS = 3
OFFLOADED = 0.55
TILE = 512
DEPTH = 4


LIMIT = 40 * 1024 * 1024


def halves(value):
    high = value.astype(jnp.bfloat16)
    low = (value - high.astype(jnp.float32)).astype(jnp.bfloat16)
    return high, low


def dot(left, right):
    return jnp.dot(left, right, preferred_element_type=jnp.float32)


def cost_of(rows, columns, members):
    return pl.CostEstimate(
        flops=8 * rows * columns * members,
        bytes_accessed=4 * (rows * columns + columns * members + rows * members),
        transcendentals=0,
    )


def stream_scratch(rows, tile):
    return [pltpu.VMEM((DEPTH, rows, tile), jnp.float32), pltpu.SemaphoreType.DMA((DEPTH,))]


def stream(design, buffer, arrived, first, steps):
    tile = buffer.shape[2]
    step = pl.program_id(0)

    def fetch(k):
        slot = lax.rem(k, DEPTH)
        return pltpu.make_async_copy(
            design.at[:, pl.ds(pl.multiple_of(first + k * tile, 128), tile)],
            buffer.at[slot],
            arrived.at[slot],
        )

    @pl.when(step == 0)
    def _():
        for k in range(min(DEPTH - 1, steps)):
            fetch(k).start()

    @pl.when(step + DEPTH - 1 < steps)
    def _():
        fetch(step + DEPTH - 1).start()

    fetch(step).wait()
    return buffer[lax.rem(step, DEPTH)]


ANYWHERE = pl.BlockSpec(memory_space=pl.ANY)


def whole_block(array):
    return pl.BlockSpec(array.shape, lambda t: (0,) * array.ndim)


def predict_kernel(first, steps, has_start, fitted, design, extra, out, total, buffer, arrived):
    members = fitted.shape[1]
    step = pl.program_id(0)
    block = stream(design, buffer, arrived, first, steps)
    right = jnp.concatenate(halves(fitted[...]), axis=1)
    term = dot(
        jnp.concatenate(halves(block), axis=1), jnp.concatenate([right, right], axis=0)
    )

    @pl.when(step == 0)
    def _():
        total[...] = term

    @pl.when(step > 0)
    def _():
        total[...] += term

    @pl.when(step == steps - 1)
    def _():
        value = total[:, :members] + total[:, members:]
        out[...] = value + extra[...] if has_start else value


def predict(design, fitted, first, tile, start=None, after=None):
    rows, (columns, members) = design.shape[0], fitted.shape
    steps = columns // tile
    extra = after if start is None else start
    return pl.pallas_call(
        functools.partial(predict_kernel, first, steps, start is not None),
        grid=(steps,),
        in_specs=[
            pl.BlockSpec((tile, members), lambda t: (t, 0)),
            ANYWHERE,
            ANYWHERE if start is None else whole_block(start),
        ],
        out_specs=pl.BlockSpec((rows, members), lambda t: (0, 0)),
        out_shape=jax.ShapeDtypeStruct((rows, members), jnp.float32),
        scratch_shapes=[pltpu.VMEM((rows, 2 * members), jnp.float32)]
        + stream_scratch(rows, tile),
        compiler_params=pltpu.CompilerParams(vmem_limit_bytes=LIMIT),
        cost_estimate=cost_of(rows, columns, members),
        name="predict",
    )(fitted, design, extra)


def stacked(value):
    return jnp.concatenate(halves(jnp.concatenate([value, value], axis=0).T), axis=0)


def gradient_tile(left, block, members):
    both = dot(left, jnp.concatenate(halves(block), axis=0))
    if both.shape[0] == 2 * members:
        both = both[:members] + both[members:]
    return both.T


def start_kernel(
    first, steps, predicted, targets, counts, design, out, influence, left, buffer, arrived
):
    members = counts.shape[1]
    block = stream(design, buffer, arrived, first, steps)

    @pl.when(pl.program_id(0) == 0)
    def _():
        residual = predicted[...] - targets[...]
        value = (
            counts[...].astype(jnp.float32) * residual / jnp.sqrt(1.0 + residual * residual)
        )
        influence[...] = value
        left[...] = stacked(value)

    out[...] = gradient_tile(left[...], block, members)


def gradient_start(predicted, targets, counts, design, first, columns, tile):
    rows, members = counts.shape
    small = (predicted, targets, counts)
    steps = columns // tile
    return pl.pallas_call(
        functools.partial(start_kernel, first, steps),
        grid=(steps,),
        in_specs=[whole_block(e) for e in small] + [ANYWHERE],
        out_specs=[
            pl.BlockSpec((tile, members), lambda t: (t, 0)),
            pl.BlockSpec((rows, members), lambda t: (0, 0)),
            pl.BlockSpec((2 * members, 2 * rows), lambda t: (0, 0)),
        ],
        out_shape=[
            jax.ShapeDtypeStruct((columns, members), jnp.float32),
            jax.ShapeDtypeStruct((rows, members), jnp.float32),
            jax.ShapeDtypeStruct((2 * members, 2 * rows), jnp.bfloat16),
        ],
        scratch_shapes=stream_scratch(rows, tile),
        compiler_params=pltpu.CompilerParams(vmem_limit_bytes=LIMIT),
        cost_estimate=cost_of(rows, columns, members),
        name="gradient_start",
    )(*small, design)


def more_kernel(first, steps, left, design, out, buffer, arrived):
    block = stream(design, buffer, arrived, first, steps)
    out[...] = gradient_tile(left[...], block, out.shape[1])


def gradient_more(left, design, first, columns, tile):
    rows, members = design.shape[0], left.shape[0] // 2
    steps = columns // tile
    return pl.pallas_call(
        functools.partial(more_kernel, first, steps),
        grid=(steps,),
        in_specs=[whole_block(left), ANYWHERE],
        out_specs=pl.BlockSpec((tile, members), lambda t: (t, 0)),
        out_shape=jax.ShapeDtypeStruct((columns, members), jnp.float32),
        scratch_shapes=stream_scratch(rows, tile),
        compiler_params=pltpu.CompilerParams(vmem_limit_bytes=LIMIT),
        cost_estimate=cost_of(rows, columns, members),
        name="gradient_more",
    )(left, design)


def squares_kernel(first, steps, counts, design, after, out, left, buffer, arrived):
    block = stream(design, buffer, arrived, first, steps)

    @pl.when(pl.program_id(0) == 0)
    def _():
        weights = counts[...].astype(jnp.float32)
        left[...] = jnp.concatenate([weights, weights], axis=0).T.astype(jnp.bfloat16)

    out[...] = gradient_tile(left[...], block * block, out.shape[1])


def squares(counts, design, first, columns, tile, after):
    rows, members = counts.shape
    steps = columns // tile
    return pl.pallas_call(
        functools.partial(squares_kernel, first, steps),
        grid=(steps,),
        in_specs=[whole_block(counts), ANYWHERE, ANYWHERE],
        out_specs=pl.BlockSpec((tile, members), lambda t: (t, 0)),
        out_shape=jax.ShapeDtypeStruct((columns, members), jnp.float32),
        scratch_shapes=[pltpu.VMEM((members, 2 * rows), jnp.bfloat16)]
        + stream_scratch(rows, tile),
        compiler_params=pltpu.CompilerParams(vmem_limit_bytes=LIMIT),
        cost_estimate=cost_of(rows, columns, members),
        name="squares",
    )(counts, design, after)


def grid_of(count):
    outer = next(k for k in range(1, count + 1) if count % k == 0 and k * k >= count)
    return outer, count // outer


def piece(array, index, rows):
    return lax.dynamic_slice_in_dim(array, index * rows, rows, 0)


def outer_perm(outer, inner, k):
    return [
        (o * inner + i, (o + k) % outer * inner + i) for o in range(outer) for i in range(inner)
    ]


def inner_perm(outer, inner, k):
    return [
        (o * inner + i, o * inner + (i + k) % inner) for o in range(outer) for i in range(inner)
    ]


def scatter_stage(array, size, place, perm_of):
    rows = array.shape[0] // size
    total = piece(array, place, rows)
    arrived = [
        lax.ppermute(piece(array, (place + k) % size, rows), "row", perm_of(k))
        for k in range(1, size)
    ]
    for term in arrived:
        total = total + term
    return total


def gather_stage(own, size, place, perm_of):
    rows = own.shape[0]
    arrived = [lax.ppermute(own, "row", perm_of(k)) for k in range(1, size)]
    line = arrived[::-1] + [own] + arrived[::-1]
    return lax.dynamic_slice_in_dim(
        jnp.concatenate(line, 0), (size - 1 - place) * rows, size * rows, 0
    )


class Permuted:
    def __init__(self, count):
        self.outer, self.inner = grid_of(count)
        index = lax.axis_index("row")
        self.o, self.i = index // self.inner, index % self.inner
        self.count = count

    def scatter(self, array):
        array = scatter_stage(
            array, self.inner, self.i, lambda k: inner_perm(self.outer, self.inner, k)
        )
        return scatter_stage(
            array, self.outer, self.o, lambda k: outer_perm(self.outer, self.inner, k)
        )

    def gather(self, own):
        own = gather_stage(own, self.outer, self.o, lambda k: outer_perm(self.outer, self.inner, k))
        return gather_stage(
            own, self.inner, self.i, lambda k: inner_perm(self.outer, self.inner, k)
        )

    def share(self, array):
        return piece(array, self.i * self.outer + self.o, array.shape[0] // self.count)


class Offloaded:
    def __init__(self, count):
        self.count = count

    def scatter(self, array):
        return lax.psum_scatter(array, "row", scatter_dimension=0, tiled=True)

    def gather(self, own):
        return lax.all_gather(own, "row", axis=0, tiled=True)

    def share(self, array):
        return piece(array, lax.axis_index("row"), array.shape[0] // self.count)


def basis_sum(value):
    count = lax.axis_size("basis")
    if count & (count - 1) or count < 2 or value.shape[0] % 16:
        return lax.psum(value, "basis")
    place = lax.axis_index("basis") % 2
    half = value.shape[0] // 2

    def across(array, bit):
        return lax.ppermute(array, "basis", [(b, b ^ bit) for b in range(count)])

    own = piece(value, place, half) + across(piece(value, 1 - place, half), 1)
    bit = 2
    while bit < count:
        own = own + across(own, bit)
        bit *= 2
    other = across(own, 1)
    return jnp.where(
        place == 0, jnp.concatenate([own, other], 0), jnp.concatenate([other, own], 0)
    )


def shards(design, targets, counts, coefficients, step_size):
    rows = lax.axis_size("row")
    basis = coefficients.shape[0]
    tile = next(t for t in (TILE, 256, 128) if basis % (2 * t) == 0)
    cut = int(basis * OFFLOADED) // tile * tile
    bounds = [0, cut, cut + (basis - cut) // (2 * tile) * tile, basis]
    ways = [Offloaded(rows), Permuted(rows), Permuted(rows)]
    parts = [part for part in zip(bounds, bounds[1:], ways) if part[0] < part[1]]
    column = targets[:, None]
    squared = []
    for a, b, _ in parts:
        squared.append(
            squares(counts, design, a, b - a, tile, squared[-1] if squared else counts)
        )
    shares = [way.share(coefficients[a:b]) for a, b, way in parts]
    rates = []
    for step in range(STEPS):
        if step == 0:
            for term, (_, _, way) in zip(squared, parts):
                rates.append(step_size[None, :] / (way.scatter(term) + 0.01))
            partial_value = predict(design, coefficients, 0, tile, after=squared[-1])
        else:
            partial_value = None
            for whole, (a, _, _) in reversed(list(zip(pieces, parts))):
                partial_value = predict(design, whole, a, tile, start=partial_value, after=whole)
        predicted = basis_sum(partial_value)
        first, influence, left = gradient_start(
            predicted, column, counts, design, 0, cut, tile
        )
        terms = [first]
        for a, b, _ in parts[1:]:
            terms.append(gradient_more(left, design, a, b - a, tile))
        moved = []
        for index, (_, _, way) in list(enumerate(parts))[1:]:
            total = way.scatter(terms[index])
            moved.append(shares[index] - rates[index] * total)
        total = parts[0][2].scatter(first)
        shares = [shares[0] - rates[0] * total] + moved
        pieces = []
        for share, (_, _, way) in zip(shares, parts):
            pieces.append(way.gather(share))
    return (jnp.concatenate(pieces, 0), influence)


def solution(mesh):
    return jax.shard_map(
        shards,
        mesh=mesh,
        in_specs=(P("row", "basis"), P("row"), P("row", None), P("basis", None), P()),
        out_specs=(P("basis", None), P("row", None)),
        check_vma=False,
    )
```
